32 devices in a mesh: group: 8 (over y, x, core), blk: 4 (over z).
Axes of the slice: x: 2, y: 2, z: 4, core: 2. Of those that a mesh axis runs over, the one named last changes fastest.
Arguments:
- embeddings: bfloat16 [8192, 1024], P(('group', 'blk')), may hold values from -6 to 6
- dest_group: int32 [8192, 1], P(('group', 'blk')), may hold values from 0 to 7; in each aligned block of 256 rows (0 to 255, 256 to 511, ...) at most 64 rows name the same one
- order_rank: int32 [8192], P(('group', 'blk')), may hold values from 0 to 8191, each once
Outputs:
- best: float32 [8192], P(('group', 'blk'))
The draws below stay inside these ranges and needn't reach their ends.
Inputs may be any that keep to these rules, and one draw needn't show every extreme that they name: `dest_group`: among the 256 members of one device, at most 64 name the same cluster. `order_rank`: all values differ.
All inputs are finite; a program needn't handle non-finite values.
Results may differ from the reference program's by a relative error of at most 0.0013.
Values may be sent and summed in bfloat16 or wider, within the bound.
No kernel may reach another device: no remote copies, remote signals or barrier semaphores. Data moves between devices by JAX's collectives and lax.ppermute only.
A program may use at most 128 MiB of HBM per device.

```python
import math
import jax
import jax.numpy as jnp
import numpy as np
from jax import lax

D = 1024
ROWS_DEV = 256
CAP = 64
M = 8192
N_GROUP = 8
DEVICES = 32


def block_scale(stream_key, dims, cuts, low, top_value):
    def one(position, parts):
        draws = jax.random.uniform(jax.random.fold_in(jax.random.fold_in(stream_key, 6), position), (parts,), jnp.float32, low / len(cuts), top_value / len(cuts))
        return jnp.repeat(jnp.exp(draws), dims[position] // parts).reshape((-1,) + (1,) * (len(dims) - position - 1))

    gain = one(*cuts[0])
    for cut in cuts[1:]:
        gain = gain * one(*cut)
    return gain


def deal_out(rng, own, number, rows, count, top, most, skew):
    sequence = jax.random.permutation(rng, count)
    heavy_load, usual = load_shares(count, rows * top, most, skew, True), load_shares(count, rows * top, most, skew, False)
    places = jnp.arange(count)

    def named(tallies, offset_by):
        used = int((tallies > 0).sum())
        fixed = max(1, used // 4)
        moved = fixed + (places - fixed + offset_by * (used - fixed)) % max(1, count - fixed)
        return jnp.zeros((count,), jnp.int32).at[sequence[jnp.where(places < fixed, places, moved)]].set(jnp.asarray(tallies, jnp.int32))

    tallies = jnp.where(number % 4 == 0, named(heavy_load, number // 4), named(usual, number - number // 4 - 1))
    mixed = jax.random.permutation(jax.random.fold_in(own, 3), count)
    giver, receiver = mixed[0:count // 2 * 2:2], mixed[1:count // 2 * 2:2]
    room = jnp.minimum(tallies[giver] - 1, most - tallies[receiver]) // 2
    room = jnp.where((giver == sequence[0]) | (receiver == sequence[0]) | (tallies[receiver] == 0), 0, jnp.maximum(room, 0))
    moved = jax.random.randint(jax.random.fold_in(own, 4), (count // 2,), 0, 1 << 20) % (room + 1)
    tallies = tallies.at[giver].add(-moved).at[receiver].add(moved)
    labels = jnp.searchsorted(jnp.cumsum(tallies), jnp.arange(rows * top), side="right").astype(jnp.int32)
    table = labels.reshape(top, rows).T
    table = table[jax.random.permutation(jax.random.fold_in(own, 1), rows)]
    offset_by = jax.random.randint(jax.random.fold_in(own, 2), (rows, 1), 0, top)
    return jnp.take_along_axis(table, (jnp.arange(top)[None, :] + offset_by) % top, axis=1)


def load_shares(count, total, bound, slope, full):
    portions = [(1 << 20) // math.isqrt(standing ** slope) + 1 for standing in range(1, count + 1)]
    largest = bound if full else min(bound, max(-(-total // count), total * portions[0] // sum(portions)))
    least = 1 if total - largest >= count - 1 else 0
    holding, rest = [largest] + [least] * (count - 1), total - largest - least * (count - 1)
    while rest > 0:
        candidates = [i for i in range(1, count) if holding[i] < largest] or [i for i in range(1, count) if holding[i] < bound]
        whole, left = sum([portions[i] for i in candidates]), rest
        for i in candidates:
            addition = min(bound - holding[i], max(1, left * portions[i] // whole), rest)
            holding[i] = holding[i] + addition
            rest = rest - addition
    return np.array(holding)


def noise(own_key, extent, scale, reach, split=(), held_as=jnp.bfloat16):
    factor_of = block_scale(own_key, extent, split, -0.22, 0.18) if split else 1.0
    array = jax.random.normal(own_key, extent, jnp.float32) * scale * factor_of
    return jnp.minimum(jnp.maximum(array, -reach), reach).astype(held_as)


def setup_inputs(seed: int = 0) -> dict:
    streams_of = jax.random.split(jax.random.key(seed), 4)
    embeddings = noise(streams_of[0], (M, D), 1.0, 6.0, ((0, 32),))
    dest_group_keys = jax.random.split(jax.random.fold_in(streams_of[1], 1), M // ROWS_DEV)
    dest_group_turns = jax.random.permutation(jax.random.fold_in(streams_of[1], 3), M // ROWS_DEV)
    dest_group = jax.vmap(lambda own, number: deal_out(jax.random.fold_in(streams_of[1], 2), own, number, ROWS_DEV, N_GROUP, 1, CAP, 2))(dest_group_keys, dest_group_turns).reshape((M, 1))
    order_rank = jax.random.permutation(streams_of[2], M).astype(jnp.int32)
    return {"embeddings": embeddings, "dest_group": dest_group, "order_rank": order_rank}


def reference(embeddings, dest_group, order_rank):
    values = embeddings.astype(jnp.float32)
    unit = (values * lax.rsqrt(lax.optimization_barrier(jnp.sum(values * values, axis=1, keepdims=True)) + 1e-06)).astype(jnp.bfloat16)
    cluster_key = dest_group[:, 0]

    def one_block(block_index):
        first_row = block_index * ROWS_DEV
        query = lax.dynamic_slice_in_dim(unit, first_row, ROWS_DEV, 0)
        query_key = lax.dynamic_slice_in_dim(cluster_key, first_row, ROWS_DEV, 0)
        query_rank = lax.dynamic_slice_in_dim(order_rank, first_row, ROWS_DEV, 0)
        scores = jnp.einsum('qd,kd->qk', query.astype(jnp.float32), unit.astype(jnp.float32))
        valid = (cluster_key[None, :] == query_key[:, None]) & (order_rank[None, :] < query_rank[:, None])
        return lax.optimization_barrier(jnp.max(jnp.where(valid, scores, -1.0), axis=1))
    result = lax.map(one_block, jnp.arange(DEVICES, dtype=jnp.int32))
    return result.reshape(-1)
```

```python
import functools

import jax
import jax.numpy as jnp
from jax import lax
from jax.experimental import pallas as pl
from jax.experimental.pallas import tpu as pltpu
from jax.sharding import PartitionSpec as P


LANES = 128
META = 16
VMEM = pl.BlockSpec(memory_space=pltpu.VMEM)
F32 = jnp.float32
BF16 = jnp.bfloat16


def nt(left, right):
    return lax.dot_general(left, right, (((1,), (1,)), ((), ())), preferred_element_type=F32)


def call(body, outs, operands, flops, moved, limit, scratch=()):
    return pl.pallas_call(
        body,
        out_shape=outs,
        in_specs=[VMEM] * len(operands),
        out_specs=jax.tree.map(lambda _: VMEM, outs),
        scratch_shapes=list(scratch),
        cost_estimate=pl.CostEstimate(flops=flops, bytes_accessed=moved, transcendentals=0),
        compiler_params=pltpu.CompilerParams(vmem_limit_bytes=limit),
    )(*operands)


def gathered(emb_ref, code_ref, chip, core, chips, cap):
    rows = emb_ref.shape[0]
    clusters = max(16, 2 * chips)
    values = emb_ref[...].astype(F32)
    norm = lax.rsqrt(jnp.sum(values * values, axis=1, keepdims=True) + 1e-06)
    unit = (values * norm).astype(BF16)
    code = code_ref[...]
    dest, rank = code >> 16, code & 65535
    onehot = (lax.broadcasted_iota(jnp.int32, (clusters, rows), 0) == dest).astype(F32)
    row = lax.broadcasted_iota(jnp.int32, (rows, rows), 0)
    column = lax.broadcasted_iota(jnp.int32, (rows, rows), 1)
    before = (row < column).astype(F32).astype(BF16)
    count = jnp.dot(onehot.astype(BF16), before, preferred_element_type=F32)
    slot = jnp.sum(count * onehot, axis=0, keepdims=True).astype(jnp.int32)
    where = ((dest >> 1) ^ chip) * cap + slot
    pos = jnp.where((dest & 1) == core, where, -1)
    pick = lax.broadcasted_iota(jnp.int32, (chips * cap, rows), 0) == pos
    pick = pick.astype(F32).astype(BF16)
    digits = lax.broadcasted_iota(jnp.int32, (META, rows), 0)
    digits = jnp.where(
        digits == 0, rank >> 8, jnp.where(digits == 1, rank & 255, jnp.where(digits == 2, 1, 0))
    )
    digits = nt(digits.astype(F32).astype(BF16), pick)
    top = lax.broadcasted_iota(jnp.int32, digits.shape, 0) == 0
    digits = jnp.where(top & (digits[2:3, :] < 0.5), 256.0, digits)
    packed = jnp.dot(pick, unit, preferred_element_type=F32).astype(BF16)
    return packed, digits, where, dest


def pack_body(cap, chips, own_ref, mate_ref, own_code, mate_code, *refs):
    group = lax.axis_index("group")
    chip, core = group >> 1, group & 1
    pieces = own_ref.shape[1] // LANES
    own, own_digits, where, dest = gathered(own_ref, own_code, chip, core, chips, cap)
    mate, mate_digits, _, _ = gathered(mate_ref, mate_code, chip, core, chips, cap)
    refs[-1][...] = where * 2 + ((dest & 1) ^ core)
    for s in range(chips):
        part = slice(s * cap, (s + 1) * cap)
        for k in range(pieces):
            lanes = slice(k * LANES, (k + 1) * LANES)
            refs[s][k * LANES : k * LANES + cap, :] = own[part, lanes]
            refs[s][k * LANES + cap : (k + 1) * LANES, :] = mate[part, lanes]
        refs[s][pieces * LANES : pieces * LANES + META, :] = jnp.concatenate(
            [own_digits[:, part], mate_digits[:, part]], axis=1
        ).astype(BF16)


def join_body(*refs):
    out_ref, base = refs[-1], 0
    for ref in refs[:-1]:
        out_ref[base : base + ref.shape[0], :] = ref[...]
        base += ref.shape[0]


def unfold(refs, pieces, x_ref, column_ref, row_ref):
    size = pieces * LANES + META
    base = 0
    for ref in refs:
        for b in range(ref.shape[0] // size):
            rows = slice(base, base + LANES)
            for k in range(pieces):
                x_ref[rows, k * LANES : (k + 1) * LANES] = ref[
                    b * size + k * LANES : b * size + (k + 1) * LANES, :
                ]
            meta = ref[b * size + pieces * LANES : (b + 1) * size, :].astype(F32)
            rank = meta[0:1, :] * 256.0 + meta[1:2, :]
            row_ref[:, rows] = rank
            column_ref[rows, :] = jnp.transpose(jnp.broadcast_to(rank, (LANES, LANES)))
            base += LANES


def wide_max(scores):
    return jnp.max(scores.reshape(-1, 8, scores.shape[1]), axis=0)


def lane_max(scores):
    parts = [scores[:, i : i + LANES] for i in range(0, scores.shape[1], LANES)]
    return functools.reduce(jnp.maximum, parts)


def across(column, width):
    return jnp.concatenate([column] * (width // LANES), axis=1)


def tile_for(count):
    return next(t for t in (512, 256, 128) if count % t == 0)


def old_body(pieces, many, *refs):
    blocks, (x_ref, column_ref, row_ref, best_ref, side_ref) = refs[:many], refs[many:]
    unfold(blocks, pieces, x_ref, column_ref, row_ref)
    count = x_ref.shape[0]
    tile = tile_for(count)
    best_ref[...] = jnp.full(best_ref.shape, -1.0, F32)
    side_ref[...] = jnp.full(side_ref.shape, -1.0, F32)

    def outer(i, _):
        mine = pl.ds(pl.multiple_of(i * tile, tile), tile)
        query, query_rank = x_ref[mine, :], row_ref[:, mine]
        scores = nt(query, query)
        earlier = across(column_ref[mine, :], tile) < query_rank
        best_ref[:, mine] = jnp.maximum(
            best_ref[:, mine], wide_max(jnp.where(earlier, scores, -1.0))
        )

        def inner(j, _):
            keys = pl.ds(pl.multiple_of(j * tile, tile), tile)
            scores = nt(x_ref[keys, :], x_ref[mine, :])
            earlier = across(column_ref[keys, :], tile) < row_ref[:, mine]
            best_ref[:, mine] = jnp.maximum(
                best_ref[:, mine], wide_max(jnp.where(earlier, scores, -1.0))
            )
            side_ref[keys, :] = jnp.maximum(
                side_ref[keys, :], lane_max(jnp.where(earlier, -1.0, scores))
            )
            return 0

        lax.fori_loop(0, i, inner, 0)
        return 0

    lax.fori_loop(0, count // tile, outer, 0)
    for i in range(0, count, LANES):
        turned = jnp.transpose(side_ref[i : i + LANES, :])
        best_ref[:, i : i + LANES] = jnp.maximum(best_ref[:, i : i + LANES], wide_max(turned))


def new_body(pieces, planes, shares, many, x_ref, column_ref, row_ref, old_ref, *refs):
    blocks, outs = refs[:many], refs[many : many + planes]
    new_ref, new_column, new_row, best_ref, side_ref, acc_ref = refs[many + planes :]
    unfold(blocks, pieces, new_ref, new_column, new_row)
    old, new = x_ref.shape[0], new_ref.shape[0]
    tile, wide = tile_for(new), tile_for(old)
    acc_ref[...] = old_ref[...]
    best_ref[...] = jnp.full(best_ref.shape, -1.0, F32)
    side_ref[...] = jnp.full(side_ref.shape, -1.0, F32)

    def outer(j, _):
        keys = pl.ds(pl.multiple_of(j * tile, tile), tile)

        def inner(i, _):
            mine = pl.ds(pl.multiple_of(i * wide, wide), wide)
            scores = nt(new_ref[keys, :], x_ref[mine, :])
            earlier = across(new_column[keys, :], wide) < row_ref[:, mine]
            acc_ref[:, mine] = jnp.maximum(
                acc_ref[:, mine], wide_max(jnp.where(earlier, scores, -1.0))
            )
            side_ref[keys, :] = jnp.maximum(
                side_ref[keys, :], lane_max(jnp.where(earlier, -1.0, scores))
            )
            return 0

        lax.fori_loop(0, old // wide, inner, 0)

        def among(i, _):
            mine = pl.ds(pl.multiple_of(i * tile, tile), tile)
            scores = nt(new_ref[keys, :], new_ref[mine, :])
            earlier = across(new_column[keys, :], tile) < new_row[:, mine]
            best_ref[:, mine] = jnp.maximum(
                best_ref[:, mine], wide_max(jnp.where(earlier, scores, -1.0))
            )
            return 0

        lax.fori_loop(0, new // tile, among, 0)
        return 0

    lax.fori_loop(0, new // tile, outer, 0)
    early, late = shares
    for p in range(planes):
        row = 0
        for start, share in ((p, 1), (planes + p * early, early)):
            for i in range(share):
                at = (start + i) * LANES
                outs[p][row : row + 1, :] = jnp.max(
                    acc_ref[:, at : at + LANES], axis=0, keepdims=True
                )
                row += 1
        for i in range(late):
            at = (p * late + i) * LANES
            side = jnp.transpose(side_ref[at : at + LANES, :])
            best = jnp.maximum(best_ref[:, at : at + LANES], wide_max(side))
            outs[p][row : row + 1, :] = jnp.max(best, axis=0, keepdims=True)
            row += 1


def final_body(cap, chips, pos_ref, own_ref, mate_ref, out_ref):
    rows = pos_ref.shape[1]
    pos = pos_ref[...]
    other, where = pos & 1, pos >> 1
    chip, slot = where // cap, where % cap
    place = lax.broadcasted_iota(jnp.int32, (LANES, rows), 0)
    pick = (place == slot + cap * other).astype(F32)
    table = jnp.concatenate([own_ref[...], mate_ref[...]], axis=0)
    got = lax.dot_general(
        table,
        pick,
        (((1,), (0,)), ((), ())),
        precision=lax.Precision.HIGHEST,
        preferred_element_type=F32,
    )
    mine = lax.broadcasted_iota(jnp.int32, (2 * chips, rows), 0) == chip + chips * other
    out_ref[...] = jnp.sum(jnp.where(mine, got, 0.0), axis=0, keepdims=True)


def on_device(embeddings, dest_group, order_rank):
    rows, width = embeddings.shape
    groups = lax.axis_size("group")
    planes = lax.axis_size("blk")
    chips, half = groups // 2, planes // 2
    cap = rows // 4
    pieces = width // LANES
    size = pieces * LANES + META
    group, plane = lax.axis_index("group"), lax.axis_index("blk")

    def blocks(n):
        return jax.ShapeDtypeStruct((n * size, LANES), BF16)

    def floats(*shape):
        return jax.ShapeDtypeStruct(shape, F32)

    def to_chip(value, s):
        return lax.ppermute(value, "group", [(i, i ^ (2 * s)) for i in range(groups)])

    def to_core(value):
        return lax.ppermute(value, "group", [(i, i ^ 1) for i in range(groups)])

    meet = [half, half - 1]
    sources = [[z for z in range(planes) if z != half]]
    sources.append([planes - 1 - z for z in sources[0]])

    def meeting(step, back=False):
        pairs = []
        for g in range(groups):
            there = g * planes + meet[g & 1]
            here = g * planes + sources[g & 1][step]
            pairs.append((there, here) if back else (here, there))
        return pairs

    def gather(value):
        arrived = [value]
        for step in range(planes - 1):
            arrived.append(lax.ppermute(value, ("group", "blk"), meeting(step)))
        return arrived

    code = (dest_group.reshape(1, rows) << 16) | order_rank.reshape(1, rows)
    mate = to_core(embeddings)
    mate_code = to_core(code)
    packed = call(
        functools.partial(pack_body, cap, chips),
        [blocks(1)] * chips + [jax.ShapeDtypeStruct((1, rows), jnp.int32)],
        [embeddings, mate, code, mate_code],
        4 * chips * cap * rows * width,
        8 * rows * width,
        16 << 20,
    )
    pos = packed[-1]
    sent = []
    for s in range(1, chips):
        sent.append(to_chip(packed[s], s))
    early = max(1, (chips - 1) * 2 // 3)
    late = chips - 1 - early

    def join(arrays):
        if len(arrays) == 1:
            return arrays[0]
        total = sum(a.shape[0] for a in arrays)
        moved = 4 * total * LANES
        out = jax.ShapeDtypeStruct((total, LANES), BF16)
        return call(join_body, out, arrays, 1000, moved, 2 * moved)

    first = gather(packed[0])
    second = gather(join(sent[:early]))
    third = gather(join(sent[early:]))
    n_old, n_new = planes * (1 + early) * LANES, planes * late * LANES

    def room(n):
        return [floats(n, LANES), floats(1, n), floats(8, n)]

    side = pltpu.VMEM((n_old, LANES), F32)
    old = call(
        functools.partial(old_body, pieces, 2 * planes),
        [jax.ShapeDtypeStruct((n_old, width), BF16)] + room(n_old),
        first + second,
        n_old * n_old * width,
        4 * n_old * width,
        6 * n_old * width,
        scratch=[side],
    )
    held = [pltpu.VMEM((n_new, width), BF16)]
    held += [pltpu.VMEM(s, F32) for s in ((n_new, LANES), (1, n_new), (8, n_new), (n_new, LANES))]
    held.append(pltpu.VMEM((8, n_old), F32))
    best = call(
        functools.partial(new_body, pieces, planes, (early, late), planes),
        [floats(chips, LANES)] * planes,
        list(old) + third,
        2 * n_new * (n_old + n_new) * width,
        2 * (n_old + n_new) * width,
        6 * (n_old + n_new) * width,
        scratch=held,
    )
    returned = [
        lax.ppermute(best[1 + step], ("group", "blk"), meeting(step, back=True))
        for step in range(planes - 1)
    ]
    at_meeting = plane == jnp.where((group & 1) == 0, half, half - 1)
    mine = jnp.where(at_meeting, best[0], functools.reduce(jnp.add, returned))
    rows_of = [mine[0:1]] + [to_chip(mine, s)[s : s + 1] for s in range(1, chips)]
    table = jnp.concatenate(rows_of, axis=0)
    result = call(
        functools.partial(final_body, cap, chips),
        floats(1, rows),
        [pos, table, to_core(table)],
        1000000,
        100000,
        4 << 20,
    )
    return result.reshape(rows)


def solution(mesh):
    placed = (P(("group", "blk"), None), P(("group", "blk"), None), P(("group", "blk")))

    return jax.shard_map(
        on_device, mesh=mesh, in_specs=placed, out_specs=P(("group", "blk")), check_vma=False
    )
```

```python
import functools

import jax
import jax.numpy as jnp
from jax import lax
from jax.experimental import pallas as pl
from jax.experimental.pallas import tpu as pltpu
from jax.sharding import PartitionSpec as P


LANES = 128
META = 16
VMEM = pl.BlockSpec(memory_space=pltpu.VMEM)
F32 = jnp.float32
BF16 = jnp.bfloat16


def nt(left, right):
    return lax.dot_general(left, right, (((1,), (1,)), ((), ())), preferred_element_type=F32)


def call(body, outs, operands, flops, moved, limit, scratch=(), spec=VMEM):
    return pl.pallas_call(
        body,
        out_shape=outs,
        in_specs=[spec] * len(operands),
        out_specs=jax.tree.map(lambda _: VMEM, outs),
        scratch_shapes=list(scratch),
        cost_estimate=pl.CostEstimate(flops=flops, bytes_accessed=moved, transcendentals=0),
        compiler_params=pltpu.CompilerParams(vmem_limit_bytes=limit),
    )(*operands)


def gathered(emb_ref, dest_ref, rank_ref, chip, core, chips, cap):
    rows = emb_ref.shape[0]
    clusters = max(16, 2 * chips)
    values = emb_ref[...].astype(F32)
    norm = lax.rsqrt(jnp.sum(values * values, axis=1, keepdims=True) + 1e-06)
    unit = (values * norm).astype(BF16)
    dest, rank = dest_ref[...], rank_ref[...]
    onehot = (lax.broadcasted_iota(jnp.int32, (clusters, rows), 0) == dest).astype(F32)
    row = lax.broadcasted_iota(jnp.int32, (rows, rows), 0)
    column = lax.broadcasted_iota(jnp.int32, (rows, rows), 1)
    before = (row < column).astype(F32).astype(BF16)
    count = jnp.dot(onehot.astype(BF16), before, preferred_element_type=F32)
    slot = jnp.sum(count * onehot, axis=0, keepdims=True).astype(jnp.int32)
    where = ((dest >> 1) ^ chip) * cap + slot
    pos = jnp.where((dest & 1) == core, where, -1)
    pick = lax.broadcasted_iota(jnp.int32, (chips * cap, rows), 0) == pos
    pick = pick.astype(F32).astype(BF16)
    digits = lax.broadcasted_iota(jnp.int32, (META, rows), 0)
    digits = jnp.where(
        digits == 0, rank >> 8, jnp.where(digits == 1, rank & 255, jnp.where(digits == 2, 1, 0))
    )
    digits = nt(digits.astype(F32).astype(BF16), pick)
    top = lax.broadcasted_iota(jnp.int32, digits.shape, 0) == 0
    digits = jnp.where(top & (digits[2:3, :] < 0.5), 256.0, digits)
    packed = jnp.dot(pick, unit, preferred_element_type=F32).astype(BF16)
    return packed, digits, where, dest


def own_body(cap, chips, emb_hbm, dest_hbm, rank_hbm, *refs):
    packed_ref, digits_ref, pos_ref, emb_ref, dest_ref, rank_ref, sems = refs
    copies = [
        pltpu.make_async_copy(source, target, sems.at[i])
        for i, (source, target) in enumerate(
            ((emb_hbm, emb_ref), (dest_hbm, dest_ref), (rank_hbm, rank_ref))
        )
    ]
    for copy in copies:
        copy.start()
    for copy in copies:
        copy.wait()
    group = lax.axis_index("group")
    packed, digits, where, dest = gathered(
        emb_ref, dest_ref, rank_ref, group >> 1, group & 1, chips, cap
    )
    packed_ref[...] = packed
    digits_ref[...] = digits
    pos_ref[...] = where * 2 + ((dest & 1) ^ (group & 1))


def pack_body(cap, chips, emb_ref, dest_ref, rank_ref, own, own_digits, *refs):
    group = lax.axis_index("group")
    pieces = emb_ref.shape[1] // LANES
    mate, mate_digits, _, _ = gathered(
        emb_ref, dest_ref, rank_ref, group >> 1, group & 1, chips, cap
    )
    for s in range(chips):
        part = slice(s * cap, (s + 1) * cap)
        for k in range(pieces):
            lanes = slice(k * LANES, (k + 1) * LANES)
            refs[s][k * LANES : k * LANES + cap, :] = own[part, lanes]
            refs[s][k * LANES + cap : (k + 1) * LANES, :] = mate[part, lanes]
        refs[s][pieces * LANES : pieces * LANES + META, :] = jnp.concatenate(
            [own_digits[:, part], mate_digits[:, part]], axis=1
        ).astype(BF16)


def join_body(*refs):
    out_ref, base = refs[-1], 0
    for ref in refs[:-1]:
        out_ref[base : base + ref.shape[0], :] = ref[...]
        base += ref.shape[0]


def unfold(refs, pieces, x_ref, column_ref, row_ref):
    size = pieces * LANES + META
    base = 0
    for ref in refs:
        for b in range(ref.shape[0] // size):
            rows = slice(base, base + LANES)
            for k in range(pieces):
                x_ref[rows, k * LANES : (k + 1) * LANES] = ref[
                    b * size + k * LANES : b * size + (k + 1) * LANES, :
                ]
            meta = ref[b * size + pieces * LANES : (b + 1) * size, :].astype(F32)
            rank = meta[0:1, :] * 256.0 + meta[1:2, :]
            row_ref[:, rows] = rank
            column_ref[rows, :] = jnp.transpose(jnp.broadcast_to(rank, (LANES, LANES)))
            base += LANES


def wide_max(scores):
    return jnp.max(scores.reshape(-1, 8, scores.shape[1]), axis=0)


def lane_max(scores):
    parts = [scores[:, i : i + LANES] for i in range(0, scores.shape[1], LANES)]
    return functools.reduce(jnp.maximum, parts)


def across(column, width):
    return jnp.concatenate([column] * (width // LANES), axis=1)


def tile_for(count):
    return next(t for t in (512, 256, 128) if count % t == 0)


def fold(keys_ref, rank_ref, best_ref, side_ref, query_ref, query_rank, symmetric):
    tall, wide = tile_for(keys_ref.shape[0]), tile_for(query_ref.shape[0])

    def outer(i, _):
        mine = pl.ds(pl.multiple_of(i * wide, wide), wide)

        def inner(j, _):
            keys = pl.ds(pl.multiple_of(j * tall, tall), tall)
            scores = nt(keys_ref[keys, :], query_ref[mine, :])
            earlier = across(rank_ref[keys, :], wide) < query_rank[:, mine]
            best_ref[:, mine] = jnp.maximum(
                best_ref[:, mine], wide_max(jnp.where(earlier, scores, -1.0))
            )
            if symmetric:
                side_ref[keys, :] = jnp.maximum(
                    side_ref[keys, :], lane_max(jnp.where(earlier, -1.0, scores))
                )
            return 0

        loop(keys_ref.shape[0] // tall, inner)
        return 0

    loop(query_ref.shape[0] // wide, outer)


def loop(count, body):
    if count == 1:
        body(0, 0)
    else:
        lax.fori_loop(0, count, body, 0)


def stage_body(pieces, olds, many, places, *refs):
    refs = list(refs)

    def take(n):
        taken = refs[:n]
        del refs[:n]
        return taken

    xs, rows, blocks = take(olds), take(olds), take(many)
    found = take(sum(range(olds + 1))) if places else []
    if places:
        outs = take(len(places))
        news, (x_ref, row_ref, best_ref) = take(olds), take(3)
    else:
        x_ref, row_ref, best_ref = take(3)
        news = take(olds)
    column_ref, side_ref = take(2)
    unfold(blocks, pieces, x_ref, column_ref, row_ref)
    best_ref[...] = jnp.full(best_ref.shape, -1.0, F32)
    side_ref[...] = jnp.full(side_ref.shape, -1.0, F32)
    for x, row, new in zip(xs, rows, news):
        new[...] = jnp.full(new.shape, -1.0, F32)
        fold(x_ref, column_ref, new, side_ref, x, row, True)
    fold(x_ref, column_ref, best_ref, side_ref, x_ref, row_ref, False)
    if not places:
        for i in range(0, x_ref.shape[0], LANES):
            side = jnp.transpose(side_ref[i : i + LANES, :])
            best_ref[:, i : i + LANES] = jnp.maximum(best_ref[:, i : i + LANES], wide_max(side))
        return
    for out, place in zip(outs, places):
        for row, (stage, block) in enumerate(place):
            lanes = slice(block * LANES, (block + 1) * LANES)
            if stage == olds:
                side = jnp.transpose(side_ref[lanes, :])
                best = jnp.maximum(best_ref[:, lanes], wide_max(side))
            else:
                best = news[stage][:, lanes]
                for later in range(stage, olds):
                    best = jnp.maximum(best, found[sum(range(later + 1)) + stage][:, lanes])
            out[row : row + 1, :] = jnp.max(best, axis=0, keepdims=True)


def final_body(cap, chips, pos_ref, own_ref, mate_ref, out_ref):
    rows = pos_ref.shape[1]
    pos = pos_ref[...]
    other, where = pos & 1, pos >> 1
    chip, slot = where // cap, where % cap
    place = lax.broadcasted_iota(jnp.int32, (LANES, rows), 0)
    pick = (place == slot + cap * other).astype(F32)
    table = jnp.concatenate([own_ref[...], mate_ref[...]], axis=0)
    got = lax.dot_general(
        table,
        pick,
        (((1,), (0,)), ((), ())),
        precision=lax.Precision.HIGHEST,
        preferred_element_type=F32,
    )
    mine = lax.broadcasted_iota(jnp.int32, (2 * chips, rows), 0) == chip + chips * other
    out_ref[...] = jnp.sum(jnp.where(mine, got, 0.0), axis=0, keepdims=True)


def chunks_of(chips):
    away = list(range(1, chips))
    cuts = [len(away) * i // 3 for i in range(4)]
    return [[0]] + [away[a:b] for a, b in zip(cuts, cuts[1:])]


def on_device(embeddings, dest_group, order_rank):
    rows, width = embeddings.shape
    groups = lax.axis_size("group")
    planes = lax.axis_size("blk")
    chips, half = groups // 2, planes // 2
    cap = rows // 4
    pieces = width // LANES
    size = pieces * LANES + META
    group, plane = lax.axis_index("group"), lax.axis_index("blk")

    def blocks(n):
        return jax.ShapeDtypeStruct((n * size, LANES), BF16)

    def floats(*shape):
        return jax.ShapeDtypeStruct(shape, F32)

    def to_chip(value, s):
        return lax.ppermute(value, "group", [(i, i ^ (2 * s)) for i in range(groups)])

    def to_core(value):
        return lax.ppermute(value, "group", [(i, i ^ 1) for i in range(groups)])

    meet = [half, half - 1]
    sources = [[z for z in range(planes) if z != half]]
    sources.append([planes - 1 - z for z in sources[0]])

    def meeting(step, back=False):
        pairs = []
        for g in range(groups):
            there = g * planes + meet[g & 1]
            here = g * planes + sources[g & 1][step]
            pairs.append((there, here) if back else (here, there))
        return pairs

    def gather(value):
        arrived = [value]
        for step in range(planes - 1):
            arrived.append(lax.ppermute(value, ("group", "blk"), meeting(step)))
        return arrived

    dest, rank = dest_group.reshape(1, rows), order_rank.reshape(1, rows)
    mate = to_core(embeddings)
    mate_dest, mate_rank = to_core(dest), to_core(rank)
    flops = 2 * chips * cap * rows * width
    own = call(
        functools.partial(own_body, cap, chips),
        [
            jax.ShapeDtypeStruct((chips * cap, width), BF16),
            floats(META, chips * cap),
            jax.ShapeDtypeStruct((1, rows), jnp.int32),
        ],
        [embeddings, dest, rank],
        flops,
        4 * rows * width,
        16 << 20,
        scratch=[
            pltpu.VMEM((rows, width), BF16),
            pltpu.VMEM((1, rows), jnp.int32),
            pltpu.VMEM((1, rows), jnp.int32),
            pltpu.SemaphoreType.DMA((3,)),
        ],
        spec=pl.BlockSpec(memory_space=pltpu.HBM),
    )
    packed = call(
        functools.partial(pack_body, cap, chips),
        [blocks(1)] * chips,
        [mate, mate_dest, mate_rank, own[0], own[1]],
        flops,
        8 * rows * width,
        16 << 20,
    )
    pos = own[2]
    sent = [packed[0]]
    for s in range(1, chips):
        sent.append(to_chip(packed[s], s))

    def join(arrays):
        if len(arrays) == 1:
            return arrays[0]
        total = sum(a.shape[0] for a in arrays)
        moved = 4 * total * LANES
        out = jax.ShapeDtypeStruct((total, LANES), BF16)
        return call(join_body, out, arrays, 1000, moved, 2 * moved)

    chunks = chunks_of(chips)
    arrived = []
    for chunk in chunks:
        arrived.append(gather(join([sent[s] for s in chunk])))
    stages = [[(c, p) for p in range(planes)] for c in range(len(chunks) - 1)]
    last = [(len(chunks) - 1, p) for p in range(planes)]
    stages += [last[:1] + last[1 + half :], last[1 : 1 + half]]
    places = [[None] * chips for _ in range(planes)]
    for i, stage in enumerate(stages):
        block = 0
        for c, p in stage:
            for s in chunks[c]:
                places[p][s] = (i, block)
                block += 1
    xs, ranks, found = [], [], []
    for i, stage in enumerate(stages):
        n = sum(len(chunks[c]) for c, _ in stage) * LANES
        flops = 2 * n * width * (n + sum(x.shape[0] for x in xs))
        made = [((n, width), BF16), ((1, n), F32), ((8, n), F32)]
        kept = [((8, x.shape[0]), F32) for x in xs]
        spare = [pltpu.VMEM((n, LANES), F32)] * 2
        operands = xs + ranks + [arrived[c][p] for c, p in stage]
        if i == len(stages) - 1:
            operands += found
            outs = [floats(chips, LANES)] * planes
            spare = [pltpu.VMEM(*m) for m in kept + made] + spare
        else:
            outs = [jax.ShapeDtypeStruct(*m) for m in made + kept]
        best = call(
            functools.partial(
                stage_body, pieces, i, len(stage), places if i == len(stages) - 1 else None
            ),
            outs,
            operands,
            flops,
            2 * width * (n + sum(x.shape[0] for x in xs)),
            6 * width * 2 * n + (12 << 20),
            scratch=spare,
        )
        if i < len(stages) - 1:
            xs.append(best[0])
            ranks.append(best[1])
            found += best[3:] + best[2:3]
    returned = [
        lax.ppermute(best[1 + step], ("group", "blk"), meeting(step, back=True))
        for step in range(planes - 1)
    ]
    at_meeting = plane == jnp.where((group & 1) == 0, half, half - 1)
    mine = jnp.where(at_meeting, best[0], functools.reduce(jnp.add, returned))
    rows_of = {(0, s): mine[s : s + 1] for s in range(chips)}
    for step in range(chips.bit_length() - 1):
        bit = 1 << step
        keys = sorted(key for key in rows_of if key[1] & bit)
        got = to_chip(jnp.concatenate([rows_of.pop(key) for key in keys], axis=0), bit)
        for i, (t, s) in enumerate(keys):
            rows_of[t ^ bit, s ^ bit] = got[i : i + 1]
    table = jnp.concatenate([rows_of[t, 0] for t in range(chips)], axis=0)
    result = call(
        functools.partial(final_body, cap, chips),
        floats(1, rows),
        [pos, table, to_core(table)],
        1000000,
        100000,
        4 << 20,
    )
    return result.reshape(rows)


def solution(mesh):
    placed = (P(("group", "blk"), None), P(("group", "blk"), None), P(("group", "blk")))

    return jax.shard_map(
        on_device, mesh=mesh, in_specs=placed, out_specs=P(("group", "blk")), check_vma=False
    )
```

```python
import functools

import jax
import jax.numpy as jnp
from jax import lax
from jax.experimental import pallas as pl
from jax.experimental.pallas import tpu as pltpu
from jax.sharding import PartitionSpec as P


LANES = 128
META = 16
VMEM = pl.BlockSpec(memory_space=pltpu.VMEM)
F32 = jnp.float32
BF16 = jnp.bfloat16


def nt(left, right):
    return lax.dot_general(left, right, (((1,), (1,)), ((), ())), preferred_element_type=F32)


def call(body, outs, operands, flops, moved, limit, scratch=(), spec=VMEM):
    return pl.pallas_call(
        body,
        out_shape=outs,
        in_specs=[spec] * len(operands),
        out_specs=jax.tree.map(lambda _: VMEM, outs),
        scratch_shapes=list(scratch),
        cost_estimate=pl.CostEstimate(flops=flops, bytes_accessed=moved, transcendentals=0),
        compiler_params=pltpu.CompilerParams(vmem_limit_bytes=limit),
    )(*operands)


def gathered(emb_ref, dest_ref, rank_ref, chip, core, chips, cap):
    rows = emb_ref.shape[0]
    clusters = max(16, 2 * chips)
    values = emb_ref[...].astype(F32)
    norm = lax.rsqrt(jnp.sum(values * values, axis=1, keepdims=True) + 1e-06)
    unit = (values * norm).astype(BF16)
    dest, rank = dest_ref[...], rank_ref[...]
    onehot = (lax.broadcasted_iota(jnp.int32, (clusters, rows), 0) == dest).astype(F32)
    row = lax.broadcasted_iota(jnp.int32, (rows, rows), 0)
    column = lax.broadcasted_iota(jnp.int32, (rows, rows), 1)
    before = (row < column).astype(F32).astype(BF16)
    count = jnp.dot(onehot.astype(BF16), before, preferred_element_type=F32)
    slot = jnp.sum(count * onehot, axis=0, keepdims=True).astype(jnp.int32)
    where = ((dest >> 1) ^ chip) * cap + slot
    pos = jnp.where((dest & 1) == core, where, -1)
    pick = lax.broadcasted_iota(jnp.int32, (chips * cap, rows), 0) == pos
    pick = pick.astype(F32).astype(BF16)
    digits = lax.broadcasted_iota(jnp.int32, (META, rows), 0)
    digits = jnp.where(
        digits == 0, rank >> 8, jnp.where(digits == 1, rank & 255, jnp.where(digits == 2, 1, 0))
    )
    digits = nt(digits.astype(F32).astype(BF16), pick)
    top = lax.broadcasted_iota(jnp.int32, digits.shape, 0) == 0
    digits = jnp.where(top & (digits[2:3, :] < 0.5), 256.0, digits)
    packed = jnp.dot(pick, unit, preferred_element_type=F32).astype(BF16)
    return packed, digits, where, dest


def own_body(cap, chips, planes, emb_hbm, dest_hbm, rank_hbm, *refs):
    packed_ref, digits_ref, pos_ref, emb_ref, dest_ref, rank_ref, sems = refs
    copies = [
        pltpu.make_async_copy(source, target, sems.at[i])
        for i, (source, target) in enumerate(
            ((emb_hbm, emb_ref), (dest_hbm, dest_ref), (rank_hbm, rank_ref))
        )
    ]
    for copy in copies:
        copy.start()
    for copy in copies:
        copy.wait()
    group = lax.axis_index("group")
    packed, digits, where, dest = gathered(
        emb_ref, dest_ref, rank_ref, group >> 1, group & 1, chips, cap
    )
    packed_ref[...] = packed
    digits_ref[...] = digits
    parity = dest & 1
    row, lane = dest * planes + planes // 2 - parity, where % cap + cap * (parity ^ (group & 1))
    pos_ref[...] = row * LANES + lane


def pack_body(cap, chips, emb_ref, dest_ref, rank_ref, own, own_digits, *refs):
    group = lax.axis_index("group")
    pieces = emb_ref.shape[1] // LANES
    mate, mate_digits, _, _ = gathered(
        emb_ref, dest_ref, rank_ref, group >> 1, group & 1, chips, cap
    )
    for s in range(chips):
        part = slice(s * cap, (s + 1) * cap)
        for k in range(pieces):
            lanes = slice(k * LANES, (k + 1) * LANES)
            refs[s][k * LANES : k * LANES + cap, :] = own[part, lanes]
            refs[s][k * LANES + cap : (k + 1) * LANES, :] = mate[part, lanes]
        refs[s][pieces * LANES : pieces * LANES + META, :] = jnp.concatenate(
            [own_digits[:, part], mate_digits[:, part]], axis=1
        ).astype(BF16)


def join_body(*refs):
    out_ref, base = refs[-1], 0
    for ref in refs[:-1]:
        out_ref[base : base + ref.shape[0], :] = ref[...]
        base += ref.shape[0]


def unfold(refs, pieces, x_ref, column_ref, row_ref):
    size = pieces * LANES + META
    base = 0
    for ref in refs:
        for b in range(ref.shape[0] // size):
            rows = slice(base, base + LANES)
            for k in range(pieces):
                x_ref[rows, k * LANES : (k + 1) * LANES] = ref[
                    b * size + k * LANES : b * size + (k + 1) * LANES, :
                ]
            meta = ref[b * size + pieces * LANES : (b + 1) * size, :].astype(F32)
            rank = meta[0:1, :] * 256.0 + meta[1:2, :]
            row_ref[:, rows] = rank
            column_ref[rows, :] = jnp.transpose(jnp.broadcast_to(rank, (LANES, LANES)))
            base += LANES


def wide_max(scores):
    return jnp.max(scores.reshape(-1, 8, scores.shape[1]), axis=0)


def lane_max(scores):
    parts = [scores[:, i : i + LANES] for i in range(0, scores.shape[1], LANES)]
    return functools.reduce(jnp.maximum, parts)


def across(column, width):
    return jnp.concatenate([column] * (width // LANES), axis=1)


def tile_for(count):
    return next(t for t in (512, 256, 128) if count % t == 0)


def fold(keys_ref, rank_ref, best_ref, side_ref, query_ref, query_rank, symmetric):
    tall, wide = tile_for(keys_ref.shape[0]), tile_for(query_ref.shape[0])

    def outer(i, _):
        mine = pl.ds(pl.multiple_of(i * wide, wide), wide)

        def inner(j, _):
            keys = pl.ds(pl.multiple_of(j * tall, tall), tall)
            scores = nt(keys_ref[keys, :], query_ref[mine, :])
            earlier = across(rank_ref[keys, :], wide) < query_rank[:, mine]
            best_ref[:, mine] = jnp.maximum(
                best_ref[:, mine], wide_max(jnp.where(earlier, scores, -1.0))
            )
            if symmetric:
                side_ref[keys, :] = jnp.maximum(
                    side_ref[keys, :], lane_max(jnp.where(earlier, -1.0, scores))
                )
            return 0

        loop(keys_ref.shape[0] // tall, inner)
        return 0

    loop(query_ref.shape[0] // wide, outer)


def loop(count, body):
    if count == 1:
        body(0, 0)
    else:
        lax.fori_loop(0, count, body, 0)


def stage_body(pieces, olds, many, places, sources, *refs):
    refs = list(refs)

    def take(n):
        taken = refs[:n]
        del refs[:n]
        return taken

    xs, rows, blocks = take(olds), take(olds), take(many)
    found = take(sum(range(olds + 1))) if places else []
    if places:
        (out,) = take(1)
        news, (x_ref, row_ref, best_ref) = take(olds), take(3)
    else:
        x_ref, row_ref, best_ref = take(3)
        news = take(olds)
    column_ref, side_ref = take(2)
    unfold(blocks, pieces, x_ref, column_ref, row_ref)
    best_ref[...] = jnp.full(best_ref.shape, -1.0, F32)
    side_ref[...] = jnp.full(side_ref.shape, -1.0, F32)
    for x, row, new in zip(xs, rows, news):
        new[...] = jnp.full(new.shape, -1.0, F32)
        fold(x_ref, column_ref, new, side_ref, x, row, True)
    fold(x_ref, column_ref, best_ref, side_ref, x_ref, row_ref, False)
    if not places:
        for i in range(0, x_ref.shape[0], LANES):
            side = jnp.transpose(side_ref[i : i + LANES, :])
            best_ref[:, i : i + LANES] = jnp.maximum(best_ref[:, i : i + LANES], wide_max(side))
        return
    planes = len(places)
    group = lax.axis_index("group")
    for p, place in enumerate(places):
        plane = jnp.where((group & 1) == 0, sources[0][p], sources[1][p])
        for s, (stage, block) in enumerate(place):
            lanes = slice(block * LANES, (block + 1) * LANES)
            if stage == olds:
                side = jnp.transpose(side_ref[lanes, :])
                best = jnp.maximum(best_ref[:, lanes], wide_max(side))
            else:
                best = news[stage][:, lanes]
                for later in range(stage, olds):
                    best = jnp.maximum(best, found[sum(range(later + 1)) + stage][:, lanes])
            best = jnp.max(best, axis=0, keepdims=True)
            device = ((group >> 1) ^ s) * 2 * planes + plane
            out[pl.ds(device, 1), :] = best
            out[pl.ds(device + planes, 1), :] = best


def final_body(pos_ref, table_ref, out_ref):
    rows, pos = pos_ref.shape[1], pos_ref[...]
    pick = lax.broadcasted_iota(jnp.int32, (LANES, rows), 0) == pos % LANES
    got = lax.dot_general(
        table_ref[...],
        pick.astype(F32),
        (((1,), (0,)), ((), ())),
        precision=lax.Precision.HIGHEST,
        preferred_element_type=F32,
    )
    mine = lax.broadcasted_iota(jnp.int32, got.shape, 0) == pos // LANES
    out_ref[...] = jnp.sum(jnp.where(mine, got, 0.0), axis=0, keepdims=True)


def chunks_of(chips):
    away = list(range(1, chips))
    cuts = [len(away) * i // 3 for i in range(4)]
    return [[0]] + [away[a:b] for a, b in zip(cuts, cuts[1:])]


def on_device(embeddings, dest_group, order_rank):
    rows, width = embeddings.shape
    groups = lax.axis_size("group")
    planes = lax.axis_size("blk")
    chips, half = groups // 2, planes // 2
    cap = rows // 4
    pieces = width // LANES
    size = pieces * LANES + META

    def blocks(n):
        return jax.ShapeDtypeStruct((n * size, LANES), BF16)

    def floats(*shape):
        return jax.ShapeDtypeStruct(shape, F32)

    def to_chip(value, s):
        return lax.ppermute(value, "group", [(i, i ^ (2 * s)) for i in range(groups)])

    def to_core(value):
        return lax.ppermute(value, "group", [(i, i ^ 1) for i in range(groups)])

    meet = [half, half - 1]
    sources = [[z for z in range(planes) if z != half]]
    sources.append([planes - 1 - z for z in sources[0]])

    def meeting(step):
        return [
            (g * planes + sources[g & 1][step], g * planes + meet[g & 1]) for g in range(groups)
        ]

    def gather(value):
        arrived = [value]
        for step in range(planes - 1):
            arrived.append(lax.ppermute(value, ("group", "blk"), meeting(step)))
        return arrived

    dest, rank = dest_group.reshape(1, rows), order_rank.reshape(1, rows)
    mate = to_core(embeddings)
    mate_dest, mate_rank = to_core(dest), to_core(rank)
    flops = 2 * chips * cap * rows * width
    own = call(
        functools.partial(own_body, cap, chips, planes),
        [
            jax.ShapeDtypeStruct((chips * cap, width), BF16),
            floats(META, chips * cap),
            jax.ShapeDtypeStruct((1, rows), jnp.int32),
        ],
        [embeddings, dest, rank],
        flops,
        4 * rows * width,
        16 << 20,
        scratch=[
            pltpu.VMEM((rows, width), BF16),
            pltpu.VMEM((1, rows), jnp.int32),
            pltpu.VMEM((1, rows), jnp.int32),
            pltpu.SemaphoreType.DMA((3,)),
        ],
        spec=pl.BlockSpec(memory_space=pltpu.HBM),
    )
    packed = call(
        functools.partial(pack_body, cap, chips),
        [blocks(1)] * chips,
        [mate, mate_dest, mate_rank, own[0], own[1]],
        flops,
        8 * rows * width,
        16 << 20,
    )
    pos = own[2]
    sent = [packed[0]]
    for s in range(1, chips):
        sent.append(to_chip(packed[s], s))

    def join(arrays):
        if len(arrays) == 1:
            return arrays[0]
        total = sum(a.shape[0] for a in arrays)
        moved = 4 * total * LANES
        out = jax.ShapeDtypeStruct((total, LANES), BF16)
        return call(join_body, out, arrays, 1000, moved, 2 * moved)

    chunks = chunks_of(chips)
    arrived = []
    for chunk in chunks:
        arrived.append(gather(join([sent[s] for s in chunk])))
    stages = [[(c, p) for p in range(planes)] for c in range(len(chunks) - 1)]
    last = [(len(chunks) - 1, p) for p in range(planes)]
    stages += [last[:1] + last[1 + half :], last[1 : 1 + half]]
    places = [[None] * chips for _ in range(planes)]
    for i, stage in enumerate(stages):
        block = 0
        for c, p in stage:
            for s in chunks[c]:
                places[p][s] = (i, block)
                block += 1
    xs, ranks, found = [], [], []
    for i, stage in enumerate(stages):
        n = sum(len(chunks[c]) for c, _ in stage) * LANES
        flops = 2 * n * width * (n + sum(x.shape[0] for x in xs))
        made = [((n, width), BF16), ((1, n), F32), ((8, n), F32)]
        kept = [((8, x.shape[0]), F32) for x in xs]
        spare = [pltpu.VMEM((n, LANES), F32)] * 2
        operands = xs + ranks + [arrived[c][p] for c, p in stage]
        if i == len(stages) - 1:
            operands += found
            outs = floats(groups * planes, LANES)
            spare = [pltpu.VMEM(*m) for m in kept + made] + spare
        else:
            outs = [jax.ShapeDtypeStruct(*m) for m in made + kept]
        best = call(
            functools.partial(
                stage_body,
                pieces,
                i,
                len(stage),
                places if i == len(stages) - 1 else None,
                [[meet[parity]] + sources[parity] for parity in range(2)],
            ),
            outs,
            operands,
            flops,
            2 * width * (n + sum(x.shape[0] for x in xs)),
            6 * width * 2 * n + (12 << 20),
            scratch=spare,
        )
        if i < len(stages) - 1:
            xs.append(best[0])
            ranks.append(best[1])
            found += best[3:] + best[2:3]
    table = lax.all_to_all(best, ("group", "blk"), 0, 0, tiled=True)
    result = call(final_body, floats(1, rows), [pos, table], 1000000, 100000, 4 << 20)
    return result.reshape(rows)


def solution(mesh):
    placed = (P(("group", "blk"), None), P(("group", "blk"), None), P(("group", "blk")))

    return jax.shard_map(
        on_device, mesh=mesh, in_specs=placed, out_specs=P(("group", "blk")), check_vma=False
    )
```

```python
import functools

import jax
import jax.numpy as jnp
from jax import lax
from jax.experimental import pallas as pl
from jax.experimental.pallas import tpu as pltpu
from jax.sharding import PartitionSpec as P


LANES = 128
META = 8
VMEM = pl.BlockSpec(memory_space=pltpu.VMEM)
F32 = jnp.float32
BF16 = jnp.bfloat16


def nt(left, right):
    return lax.dot_general(left, right, (((1,), (1,)), ((), ())), preferred_element_type=F32)


def call(body, outs, operands, flops, moved, limit, scratch=(), spec=VMEM):
    return pl.pallas_call(
        body,
        out_shape=outs,
        in_specs=[spec] * len(operands),
        out_specs=jax.tree.map(lambda _: VMEM, outs),
        scratch_shapes=list(scratch),
        cost_estimate=pl.CostEstimate(flops=flops, bytes_accessed=moved, transcendentals=0),
        compiler_params=pltpu.CompilerParams(vmem_limit_bytes=limit),
    )(*operands)


def gathered(emb_ref, code_ref, chip, core, chips, cap):
    rows = emb_ref.shape[0]
    clusters = max(16, 2 * chips)
    values = emb_ref[...].astype(F32)
    norm = lax.rsqrt(jnp.sum(values * values, axis=1, keepdims=True) + 1e-06)
    unit = (values * norm).astype(BF16)
    dest, rank = code_ref[0:1, :], code_ref[1:2, :]
    onehot = (lax.broadcasted_iota(jnp.int32, (clusters, rows), 0) == dest).astype(F32)
    row = lax.broadcasted_iota(jnp.int32, (rows, rows), 0)
    column = lax.broadcasted_iota(jnp.int32, (rows, rows), 1)
    before = (row < column).astype(F32).astype(BF16)
    count = jnp.dot(onehot.astype(BF16), before, preferred_element_type=F32)
    slot = jnp.sum(count * onehot, axis=0, keepdims=True).astype(jnp.int32)
    where = ((dest >> 1) ^ chip) * cap + slot
    pos = jnp.where((dest & 1) == core, where, -1)
    pick = lax.broadcasted_iota(jnp.int32, (chips * cap, rows), 0) == pos
    pick = pick.astype(F32).astype(BF16)
    digits = lax.broadcasted_iota(jnp.int32, (2 * META, rows), 0)
    digits = jnp.where(
        digits == 0, rank >> 8, jnp.where(digits == 1, rank & 255, jnp.where(digits == 2, 1, 0))
    )
    digits = nt(digits.astype(F32).astype(BF16), pick)
    top = lax.broadcasted_iota(jnp.int32, digits.shape, 0) == 0
    digits = jnp.where(top & (digits[2:3, :] < 0.5), 256.0, digits)
    packed = jnp.dot(pick, unit, preferred_element_type=F32).astype(BF16)
    return packed, digits, where, dest


def own_body(cap, chips, emb_ref, code_ref, packed_ref, digits_ref, pos_ref):
    group = lax.axis_index("group")
    packed, digits, where, dest = gathered(emb_ref, code_ref, group >> 1, group & 1, chips, cap)
    packed_ref[...] = packed
    digits_ref[...] = digits
    parity = dest & 1
    pos_ref[...] = dest * LANES + where % cap + cap * (parity ^ (group & 1))


def pack_body(cap, chips, emb_ref, code_ref, own, own_digits, *refs):
    group = lax.axis_index("group")
    pieces = emb_ref.shape[1] // LANES
    mate, mate_digits, _, _ = gathered(emb_ref, code_ref, group >> 1, group & 1, chips, cap)
    for s in range(chips):
        part = slice(s * cap, (s + 1) * cap)
        for k in range(pieces):
            lanes = slice(k * LANES, (k + 1) * LANES)
            refs[s][k * LANES : k * LANES + cap, :] = own[part, lanes]
            refs[s][k * LANES + cap : (k + 1) * LANES, :] = mate[part, lanes]
        refs[s][pieces * LANES : pieces * LANES + META, :] = jnp.concatenate(
            [own_digits[:META, part], mate_digits[:META, part]], axis=1
        ).astype(BF16)


def join_body(*refs):
    out_ref, base = refs[-1], 0
    for ref in refs[:-1]:
        out_ref[base : base + ref.shape[0], :] = ref[...]
        base += ref.shape[0]


def unfold(refs, pieces, x_ref, column_ref, row_ref):
    size = pieces * LANES + META
    base = 0
    for ref in refs:
        for b in range(ref.shape[0] // size):
            rows = slice(base, base + LANES)
            for k in range(pieces):
                x_ref[rows, k * LANES : (k + 1) * LANES] = ref[
                    b * size + k * LANES : b * size + (k + 1) * LANES, :
                ]
            meta = ref[b * size + pieces * LANES : (b + 1) * size, :].astype(F32)
            rank = meta[0:1, :] * 256.0 + meta[1:2, :]
            row_ref[:, rows] = rank
            column_ref[rows, :] = jnp.transpose(jnp.broadcast_to(rank, (LANES, LANES)))
            base += LANES


def wide_max(scores):
    return jnp.max(scores.reshape(-1, 8, scores.shape[1]), axis=0)


def lane_max(scores):
    parts = [scores[:, i : i + LANES] for i in range(0, scores.shape[1], LANES)]
    return functools.reduce(jnp.maximum, parts)


def across(column, width):
    return jnp.concatenate([column] * (width // LANES), axis=1)


def tile_for(count):
    return next(t for t in (512, 256, 128) if count % t == 0)


def fold(keys_ref, rank_ref, best_ref, side_ref, query_ref, query_rank, symmetric):
    tall, wide = tile_for(keys_ref.shape[0]), tile_for(query_ref.shape[0])

    def outer(i, _):
        mine = pl.ds(pl.multiple_of(i * wide, wide), wide)

        def inner(j, _):
            keys = pl.ds(pl.multiple_of(j * tall, tall), tall)
            scores = nt(keys_ref[keys, :], query_ref[mine, :])
            earlier = across(rank_ref[keys, :], wide) < query_rank[:, mine]
            best_ref[:, mine] = jnp.maximum(
                best_ref[:, mine], wide_max(jnp.where(earlier, scores, -1.0))
            )
            if symmetric:
                side_ref[keys, :] = jnp.maximum(
                    side_ref[keys, :], lane_max(jnp.where(earlier, -1.0, scores))
                )
            return 0

        loop(keys_ref.shape[0] // tall, inner)
        return 0

    loop(query_ref.shape[0] // wide, outer)


def loop(count, body):
    if count == 1:
        body(0, 0)
    else:
        lax.fori_loop(0, count, body, 0)


def stage_body(pieces, olds, many, places, sources, *refs):
    refs = list(refs)

    def take(n):
        taken = refs[:n]
        del refs[:n]
        return taken

    xs, rows, blocks = take(olds), take(olds), take(many)
    found = take(sum(range(olds + 1))) if places else []
    if places:
        (out,) = take(1)
        news, (x_ref, row_ref, best_ref) = take(olds), take(3)
    else:
        x_ref, row_ref, best_ref = take(3)
        news = take(olds)
    column_ref, side_ref = take(2)
    unfold(blocks, pieces, x_ref, column_ref, row_ref)
    best_ref[...] = jnp.full(best_ref.shape, -1.0, F32)
    side_ref[...] = jnp.full(side_ref.shape, -1.0, F32)
    for x, row, new in zip(xs, rows, news):
        new[...] = jnp.full(new.shape, -1.0, F32)
        fold(x_ref, column_ref, new, side_ref, x, row, True)
    fold(x_ref, column_ref, best_ref, side_ref, x_ref, row_ref, False)
    if not places:
        for i in range(0, x_ref.shape[0], LANES):
            side = jnp.transpose(side_ref[i : i + LANES, :])
            best_ref[:, i : i + LANES] = jnp.maximum(best_ref[:, i : i + LANES], wide_max(side))
        return
    planes = len(places)
    group = lax.axis_index("group")
    for p, place in enumerate(places):
        plane = jnp.where((group & 1) == 0, sources[0][p], sources[1][p])
        for s, (stage, block) in enumerate(place):
            lanes = slice(block * LANES, (block + 1) * LANES)
            if stage == olds:
                side = jnp.transpose(side_ref[lanes, :])
                best = jnp.maximum(best_ref[:, lanes], wide_max(side))
            else:
                best = news[stage][:, lanes]
                for later in range(stage, olds):
                    best = jnp.maximum(best, found[sum(range(later + 1)) + stage][:, lanes])
            best = jnp.max(best, axis=0, keepdims=True)
            device = ((group >> 1) ^ s) * 2 * planes + plane
            out[pl.ds(device, 1), :] = best
            out[pl.ds(device + planes, 1), :] = best


def final_body(planes, pos_ref, table_ref, out_ref):
    groups = table_ref.shape[0] // planes
    pos = pos_ref[...]
    rows = [g * planes + planes // 2 - (g & 1) for g in range(groups)]
    table = jnp.concatenate([table_ref[r : r + 1, :] for r in rows], axis=0)
    for i in range(0, pos.shape[1], LANES):
        here = jnp.broadcast_to(pos[:, i : i + LANES], (groups, LANES))
        got = jnp.take_along_axis(table, here % LANES, axis=1)
        mine = lax.broadcasted_iota(jnp.int32, here.shape, 0) == here // LANES
        out_ref[:, i : i + LANES] = jnp.sum(jnp.where(mine, got, 0.0), axis=0, keepdims=True)


def chunks_of(chips):
    away = list(range(1, chips))
    cuts = [len(away) * i // 3 for i in range(4)]
    return [[0]] + [away[a:b] for a, b in zip(cuts, cuts[1:])]


def on_device(embeddings, dest_group, order_rank):
    rows, width = embeddings.shape
    groups = lax.axis_size("group")
    planes = lax.axis_size("blk")
    chips, half = groups // 2, planes // 2
    cap = rows // 4
    pieces = width // LANES
    size = pieces * LANES + META

    def blocks(n):
        return jax.ShapeDtypeStruct((n * size, LANES), BF16)

    def floats(*shape):
        return jax.ShapeDtypeStruct(shape, F32)

    def to_chip(value, s):
        return lax.ppermute(value, "group", [(i, i ^ (2 * s)) for i in range(groups)])

    def to_core(value):
        return lax.ppermute(value, "group", [(i, i ^ 1) for i in range(groups)])

    meet = [half, half - 1]
    sources = [[z for z in range(planes) if z != half]]
    sources.append([planes - 1 - z for z in sources[0]])

    def meeting(step):
        return [
            (g * planes + sources[g & 1][step], g * planes + meet[g & 1]) for g in range(groups)
        ]

    def gather(value):
        arrived = [value]
        for step in range(planes - 1):
            arrived.append(lax.ppermute(value, ("group", "blk"), meeting(step)))
        return arrived

    code = jnp.concatenate([dest_group.reshape(1, rows), order_rank.reshape(1, rows)], axis=0)
    mate = to_core(embeddings)
    mate_code = to_core(code)
    flops = 2 * chips * cap * rows * width
    own = call(
        functools.partial(own_body, cap, chips),
        [
            jax.ShapeDtypeStruct((chips * cap, width), BF16),
            floats(2 * META, chips * cap),
            jax.ShapeDtypeStruct((1, rows), jnp.int32),
        ],
        [embeddings, code],
        flops,
        4 * rows * width,
        16 << 20,
    )
    packed = call(
        functools.partial(pack_body, cap, chips),
        [blocks(1)] * chips,
        [mate, mate_code, own[0], own[1]],
        flops,
        8 * rows * width,
        16 << 20,
    )
    pos = own[2]
    sent = [packed[0]]
    for s in range(1, chips):
        sent.append(to_chip(packed[s], s))

    def join(arrays):
        if len(arrays) == 1:
            return arrays[0]
        total = sum(a.shape[0] for a in arrays)
        moved = 4 * total * LANES
        out = jax.ShapeDtypeStruct((total, LANES), BF16)
        return call(join_body, out, arrays, 1000, moved, 2 * moved)

    chunks = chunks_of(chips)
    arrived = []
    for chunk in chunks:
        arrived.append(gather(join([sent[s] for s in chunk])))
    stages = [[(c, p) for p in range(planes)] for c in range(len(chunks) - 1)]
    last = [(len(chunks) - 1, p) for p in range(planes)]
    stages += [last[:1] + last[1 + half :], last[1 : 1 + half]]
    places = [[None] * chips for _ in range(planes)]
    for i, stage in enumerate(stages):
        block = 0
        for c, p in stage:
            for s in chunks[c]:
                places[p][s] = (i, block)
                block += 1
    xs, ranks, found = [], [], []
    for i, stage in enumerate(stages):
        n = sum(len(chunks[c]) for c, _ in stage) * LANES
        flops = 2 * n * width * (n + sum(x.shape[0] for x in xs))
        made = [((n, width), BF16), ((1, n), F32), ((8, n), F32)]
        kept = [((8, x.shape[0]), F32) for x in xs]
        spare = [pltpu.VMEM((n, LANES), F32)] * 2
        operands = xs + ranks + [arrived[c][p] for c, p in stage]
        if i == len(stages) - 1:
            operands += found
            outs = floats(groups * planes, LANES)
            spare = [pltpu.VMEM(*m) for m in kept + made] + spare
        else:
            outs = [jax.ShapeDtypeStruct(*m) for m in made + kept]
        best = call(
            functools.partial(
                stage_body,
                pieces,
                i,
                len(stage),
                places if i == len(stages) - 1 else None,
                [[meet[parity]] + sources[parity] for parity in range(2)],
            ),
            outs,
            operands,
            flops,
            2 * width * (n + sum(x.shape[0] for x in xs)),
            6 * width * 2 * n + (12 << 20),
            scratch=spare,
        )
        if i < len(stages) - 1:
            xs.append(best[0])
            ranks.append(best[1])
            found += best[3:] + best[2:3]
    table = lax.all_to_all(best, ("group", "blk"), 0, 0, tiled=True)
    final = functools.partial(final_body, planes)
    result = call(final, floats(1, rows), [pos, table], 1000000, 100000, 4 << 20)
    return result.reshape(rows)


def solution(mesh):
    placed = (P(("group", "blk"), None), P(("group", "blk"), None), P(("group", "blk")))

    return jax.shard_map(
        on_device, mesh=mesh, in_specs=placed, out_specs=P(("group", "blk")), check_vma=False
    )
```

```python
import functools

import jax
import jax.numpy as jnp
from jax import lax
from jax.experimental import pallas as pl
from jax.experimental.pallas import tpu as pltpu
from jax.sharding import PartitionSpec as P


LANES = 128
META = 8
VMEM = pl.BlockSpec(memory_space=pltpu.VMEM)
F32 = jnp.float32
BF16 = jnp.bfloat16


def nt(left, right):
    return lax.dot_general(left, right, (((1,), (1,)), ((), ())), preferred_element_type=F32)


def call(body, outs, operands, flops, moved, limit, scratch=(), spec=VMEM):
    return pl.pallas_call(
        body,
        out_shape=outs,
        in_specs=[spec] * len(operands),
        out_specs=jax.tree.map(lambda _: VMEM, outs),
        scratch_shapes=list(scratch),
        cost_estimate=pl.CostEstimate(flops=flops, bytes_accessed=moved, transcendentals=0),
        compiler_params=pltpu.CompilerParams(vmem_limit_bytes=limit),
    )(*operands)


def gathered(emb_ref, code_ref, chip, core, chips, cap):
    rows = emb_ref.shape[0]
    clusters = max(16, 2 * chips)
    values = emb_ref[...].astype(F32)
    norm = lax.rsqrt(jnp.sum(values * values, axis=1, keepdims=True) + 1e-06)
    unit = (values * norm).astype(BF16)
    dest, rank = code_ref[0:1, :], code_ref[1:2, :]
    onehot = (lax.broadcasted_iota(jnp.int32, (clusters, rows), 0) == dest).astype(F32)
    row = lax.broadcasted_iota(jnp.int32, (rows, rows), 0)
    column = lax.broadcasted_iota(jnp.int32, (rows, rows), 1)
    before = (row < column).astype(F32).astype(BF16)
    count = jnp.dot(onehot.astype(BF16), before, preferred_element_type=F32)
    slot = jnp.sum(count * onehot, axis=0, keepdims=True).astype(jnp.int32)
    where = ((dest >> 1) ^ chip) * cap + slot
    pos = jnp.where((dest & 1) == core, where, -1)
    pick = lax.broadcasted_iota(jnp.int32, (chips * cap, rows), 0) == pos
    pick = pick.astype(F32).astype(BF16)
    digits = lax.broadcasted_iota(jnp.int32, (2 * META, rows), 0)
    digits = jnp.where(
        digits == 0, rank >> 8, jnp.where(digits == 1, rank & 255, jnp.where(digits == 2, 1, 0))
    )
    digits = nt(digits.astype(F32).astype(BF16), pick)
    top = lax.broadcasted_iota(jnp.int32, digits.shape, 0) == 0
    digits = jnp.where(top & (digits[2:3, :] < 0.5), 256.0, digits)
    packed = jnp.dot(pick, unit, preferred_element_type=F32).astype(BF16)
    return packed, digits, where, dest


def own_body(cap, chips, emb_ref, code_ref, packed_ref, digits_ref, pos_ref):
    group = lax.axis_index("group")
    packed, digits, where, dest = gathered(emb_ref, code_ref, group >> 1, group & 1, chips, cap)
    packed_ref[...] = packed
    digits_ref[...] = digits
    parity = dest & 1
    pos_ref[...] = dest * LANES + where % cap + cap * (parity ^ (group & 1))


def pack_body(cap, chips, emb_ref, code_ref, own, own_digits, *refs):
    group = lax.axis_index("group")
    pieces = emb_ref.shape[1] // LANES
    mate, mate_digits, _, _ = gathered(emb_ref, code_ref, group >> 1, group & 1, chips, cap)
    for s in range(chips):
        part = slice(s * cap, (s + 1) * cap)
        for k in range(pieces):
            lanes = slice(k * LANES, (k + 1) * LANES)
            refs[s][k * LANES : k * LANES + cap, :] = own[part, lanes]
            refs[s][k * LANES + cap : (k + 1) * LANES, :] = mate[part, lanes]
        refs[s][pieces * LANES : pieces * LANES + META, :] = jnp.concatenate(
            [own_digits[:META, part], mate_digits[:META, part]], axis=1
        ).astype(BF16)


def join_body(*refs):
    out_ref, base = refs[-1], 0
    for ref in refs[:-1]:
        out_ref[base : base + ref.shape[0], :] = ref[...]
        base += ref.shape[0]


def unfold(refs, pieces, x_ref, turned_ref, column_ref, row_ref):
    size = pieces * LANES + META
    base = 0
    for ref in refs:
        for b in range(ref.shape[0] // size):
            rows = slice(base, base + LANES)
            for k in range(pieces):
                lanes = slice(k * LANES, (k + 1) * LANES)
                piece = ref[b * size + k * LANES : b * size + (k + 1) * LANES, :]
                x_ref[rows, lanes] = piece
                if turned_ref is not None:
                    turned_ref[lanes, rows] = jnp.transpose(piece)
            meta = ref[b * size + pieces * LANES : (b + 1) * size, :].astype(F32)
            rank = meta[0:1, :] * 256.0 + meta[1:2, :]
            row_ref[:, rows] = rank
            column_ref[rows, :] = jnp.transpose(jnp.broadcast_to(rank, (LANES, LANES)))
            base += LANES


def wide_max(scores):
    return jnp.max(scores.reshape(-1, 8, scores.shape[1]), axis=0)


def lane_max(scores):
    parts = [scores[:, i : i + LANES] for i in range(0, scores.shape[1], LANES)]
    return functools.reduce(jnp.maximum, parts)


def across(column, width):
    return jnp.concatenate([column] * (width // LANES), axis=1)


def fold(keys_ref, rank_ref, best_ref, side_ref, query_ref, query_rank, turned):
    queries = query_rank.shape[1]
    tall = next(t for t in (512, 256, 128) if keys_ref.shape[0] % t == 0)
    wide = next(t for t in (256, 128) if queries % t == 0)

    def outer(i, _):
        mine = span(i, wide)

        def inner(j, _):
            keys = span(j, tall)
            if turned:
                scores = jnp.dot(
                    keys_ref[keys, :], query_ref[:, mine], preferred_element_type=F32
                )
            else:
                scores = nt(keys_ref[keys, :], query_ref[mine, :])
            earlier = across(rank_ref[keys, :], wide) < query_rank[:, mine]
            best_ref[:, mine] = jnp.maximum(
                best_ref[:, mine], wide_max(jnp.where(earlier, scores, -1.0))
            )
            if turned:
                side_ref[keys, :] = jnp.maximum(
                    side_ref[keys, :], lane_max(jnp.where(earlier, -1.0, scores))
                )
            return 0

        loop(keys_ref.shape[0] // tall, inner)
        return 0

    loop(queries // wide, outer)


def span(i, size):
    if isinstance(i, int):
        return slice(i * size, (i + 1) * size)
    return pl.ds(pl.multiple_of(i * size, size), size)


def loop(count, body):
    if count <= 4:
        for i in range(count):
            body(i, 0)
    else:
        lax.fori_loop(0, count, body, 0)


def stage_body(pieces, olds, many, places, sources, *refs):
    refs = list(refs)

    def take(n):
        taken = refs[:n]
        del refs[:n]
        return taken

    xs, rows, blocks = take(olds), take(olds), take(many)
    found = take(sum(range(olds + 1))) if places else []
    if places:
        (out,) = take(1)
        news, turned_ref, (row_ref, best_ref) = take(olds), None, take(2)
    else:
        turned_ref, row_ref, best_ref = take(3)
        news = take(olds)
    x_ref, column_ref, side_ref = take(3)
    unfold(blocks, pieces, x_ref, turned_ref, column_ref, row_ref)
    best_ref[...] = jnp.full(best_ref.shape, -1.0, F32)
    side_ref[...] = jnp.full(side_ref.shape, -1.0, F32)
    for x, row, new in zip(xs, rows, news):
        new[...] = jnp.full(new.shape, -1.0, F32)
        fold(x_ref, column_ref, new, side_ref, x, row, True)
    fold(x_ref, column_ref, best_ref, side_ref, x_ref, row_ref, False)
    if not places:
        for i in range(0, x_ref.shape[0], LANES):
            side = jnp.transpose(side_ref[i : i + LANES, :])
            best_ref[:, i : i + LANES] = jnp.maximum(best_ref[:, i : i + LANES], wide_max(side))
        return
    planes = len(places)
    group = lax.axis_index("group")
    for p, place in enumerate(places):
        plane = jnp.where((group & 1) == 0, sources[0][p], sources[1][p])
        for s, (stage, block) in enumerate(place):
            lanes = slice(block * LANES, (block + 1) * LANES)
            if stage == olds:
                side = jnp.transpose(side_ref[lanes, :])
                best = jnp.maximum(best_ref[:, lanes], wide_max(side))
            else:
                best = news[stage][:, lanes]
                for later in range(stage, olds):
                    best = jnp.maximum(best, found[sum(range(later + 1)) + stage][:, lanes])
            best = jnp.max(best, axis=0, keepdims=True)
            device = ((group >> 1) ^ s) * 2 * planes + plane
            out[pl.ds(device, 1), :] = best
            out[pl.ds(device + planes, 1), :] = best


def final_body(planes, pos_ref, table_ref, out_ref):
    groups = table_ref.shape[0] // planes
    pos = pos_ref[...]
    rows = [g * planes + planes // 2 - 1 + (g & 1) for g in range(groups)]
    table = jnp.concatenate([table_ref[r : r + 1, :] for r in rows], axis=0)
    for i in range(0, pos.shape[1], LANES):
        here = jnp.broadcast_to(pos[:, i : i + LANES], (groups, LANES))
        got = jnp.take_along_axis(table, here % LANES, axis=1)
        mine = lax.broadcasted_iota(jnp.int32, here.shape, 0) == here // LANES
        out_ref[:, i : i + LANES] = jnp.sum(jnp.where(mine, got, 0.0), axis=0, keepdims=True)


def chunks_of(chips):
    away = list(range(1, chips))
    cuts = [len(away) * i // 3 for i in range(4)]
    return [[0]] + [away[a:b] for a, b in zip(cuts, cuts[1:])]


def on_device(embeddings, dest_group, order_rank):
    rows, width = embeddings.shape
    groups = lax.axis_size("group")
    planes = lax.axis_size("blk")
    chips, half = groups // 2, planes // 2
    cap = rows // 4
    pieces = width // LANES
    size = pieces * LANES + META

    def blocks(n):
        return jax.ShapeDtypeStruct((n * size, LANES), BF16)

    def floats(*shape):
        return jax.ShapeDtypeStruct(shape, F32)

    def to_chip(value, s):
        return lax.ppermute(value, "group", [(i, i ^ (2 * s)) for i in range(groups)])

    def to_core(value):
        return lax.ppermute(value, "group", [(i, i ^ 1) for i in range(groups)])

    meet = [half - 1, half]
    sources = [[z for z in range(planes) if z != half]]
    sources.insert(0, [planes - 1 - z for z in sources[0]])

    def meeting(step):
        return [
            (g * planes + sources[g & 1][step], g * planes + meet[g & 1]) for g in range(groups)
        ]

    def gather(value):
        arrived = [value]
        for step in range(planes - 1):
            arrived.append(lax.ppermute(value, ("group", "blk"), meeting(step)))
        return arrived

    code = jnp.concatenate([dest_group.reshape(1, rows), order_rank.reshape(1, rows)], axis=0)
    mate = to_core(embeddings)
    mate_code = to_core(code)
    flops = 2 * chips * cap * rows * width
    own = call(
        functools.partial(own_body, cap, chips),
        [
            jax.ShapeDtypeStruct((chips * cap, width), BF16),
            floats(2 * META, chips * cap),
            jax.ShapeDtypeStruct((1, rows), jnp.int32),
        ],
        [embeddings, code],
        flops,
        4 * rows * width,
        16 << 20,
    )
    packed = call(
        functools.partial(pack_body, cap, chips),
        [blocks(1)] * chips,
        [mate, mate_code, own[0], own[1]],
        flops,
        8 * rows * width,
        16 << 20,
    )
    pos = own[2]
    sent = [packed[0]]
    for s in range(1, chips):
        sent.append(to_chip(packed[s], s))

    def join(arrays):
        if len(arrays) == 1:
            return arrays[0]
        total = sum(a.shape[0] for a in arrays)
        moved = 4 * total * LANES
        out = jax.ShapeDtypeStruct((total, LANES), BF16)
        return call(join_body, out, arrays, 1000, moved, 2 * moved)

    chunks = chunks_of(chips)
    arrived = []
    for chunk in chunks:
        arrived.append(gather(join([sent[s] for s in chunk])))
    stages = [[(c, p) for p in range(planes)] for c in range(len(chunks) - 1)]
    last = [(len(chunks) - 1, p) for p in range(planes)]
    stages += [last[:1] + last[1 + half :], last[1 : 1 + half]]
    places = [[None] * chips for _ in range(planes)]
    for i, stage in enumerate(stages):
        block = 0
        for c, p in stage:
            for s in chunks[c]:
                places[p][s] = (i, block)
                block += 1
    xs, ranks, found = [], [], []
    for i, stage in enumerate(stages):
        n = sum(len(chunks[c]) for c, _ in stage) * LANES
        count = n + sum(x.shape[1] for x in xs)
        flops = 2 * n * width * count
        made = [((width, n), BF16), ((1, n), F32), ((8, n), F32)]
        kept = [((8, x.shape[1]), F32) for x in xs]
        spare = [pltpu.VMEM((n, width), BF16)] + [pltpu.VMEM((n, LANES), F32)] * 2
        operands = xs + ranks + [arrived[c][p] for c, p in stage]
        if i == len(stages) - 1:
            operands += found
            outs = floats(groups * planes, LANES)
            spare = [pltpu.VMEM(*m) for m in kept + made[1:]] + spare
        else:
            outs = [jax.ShapeDtypeStruct(*m) for m in made + kept]
        best = call(
            functools.partial(
                stage_body,
                pieces,
                i,
                len(stage),
                places if i == len(stages) - 1 else None,
                [[meet[parity]] + sources[parity] for parity in range(2)],
            ),
            outs,
            operands,
            flops,
            2 * width * count,
            8 * width * 2 * n + (12 << 20),
            scratch=spare,
        )
        if i < len(stages) - 1:
            xs.append(best[0])
            ranks.append(best[1])
            found += best[3:] + best[2:3]
    table = lax.all_to_all(best, ("group", "blk"), 0, 0, tiled=True)
    final = functools.partial(final_body, planes)
    result = call(final, floats(1, rows), [pos, table], 1000000, 100000, 4 << 20)
    return result.reshape(rows)


def solution(mesh):
    placed = (P(("group", "blk"), None), P(("group", "blk"), None), P(("group", "blk")))

    return jax.shard_map(
        on_device, mesh=mesh, in_specs=placed, out_specs=P(("group", "blk")), check_vma=False
    )
```

```python
import functools

import jax
import jax.numpy as jnp
from jax import lax
from jax.experimental import pallas as pl
from jax.experimental.pallas import tpu as pltpu
from jax.sharding import PartitionSpec as P


LANES = 128
META = 8
VMEM = pl.BlockSpec(memory_space=pltpu.VMEM)
F32 = jnp.float32
BF16 = jnp.bfloat16


def nt(left, right):
    return lax.dot_general(left, right, (((1,), (1,)), ((), ())), preferred_element_type=F32)


def call(body, outs, operands, flops, moved, limit, scratch=(), spec=VMEM):
    return pl.pallas_call(
        body,
        out_shape=outs,
        in_specs=[spec] * len(operands),
        out_specs=jax.tree.map(lambda _: VMEM, outs),
        scratch_shapes=list(scratch),
        cost_estimate=pl.CostEstimate(flops=flops, bytes_accessed=moved, transcendentals=0),
        compiler_params=pltpu.CompilerParams(vmem_limit_bytes=limit),
    )(*operands)


def unit_of(emb_ref):
    values = emb_ref[...].astype(F32)
    norm = lax.rsqrt(jnp.sum(values * values, axis=1, keepdims=True) + 1e-06)
    return (values * norm).astype(BF16)


def picked(code_ref, chip, core, chips, cap):
    rows = code_ref.shape[1]
    clusters = max(16, 2 * chips)
    dest, rank = code_ref[0:1, :], code_ref[1:2, :]
    onehot = (lax.broadcasted_iota(jnp.int32, (clusters, rows), 0) == dest).astype(F32)
    row = lax.broadcasted_iota(jnp.int32, (rows, rows), 0)
    column = lax.broadcasted_iota(jnp.int32, (rows, rows), 1)
    before = (row < column).astype(F32).astype(BF16)
    count = jnp.dot(onehot.astype(BF16), before, preferred_element_type=F32)
    slot = jnp.sum(count * onehot, axis=0, keepdims=True).astype(jnp.int32)
    where = ((dest >> 1) ^ chip) * cap + slot
    pos = jnp.where((dest & 1) == core, where, -1)
    pick = lax.broadcasted_iota(jnp.int32, (chips * cap, rows), 0) == pos
    pick = pick.astype(F32).astype(BF16)
    digits = lax.broadcasted_iota(jnp.int32, (2 * META, rows), 0)
    digits = jnp.where(
        digits == 0, rank >> 8, jnp.where(digits == 1, rank & 255, jnp.where(digits == 2, 1, 0))
    )
    digits = nt(digits.astype(F32).astype(BF16), pick)
    top = lax.broadcasted_iota(jnp.int32, digits.shape, 0) == 0
    digits = jnp.where(top & (digits[2:3, :] < 0.5), 256.0, digits)
    return pick, digits, where, dest


def index_body(cap, chips, code_ref, pick_ref, digits_ref, pos_ref):
    group = lax.axis_index("group")
    pick, digits, where, dest = picked(code_ref, group >> 1, group & 1, chips, cap)
    pick_ref[...] = pick
    digits_ref[...] = digits
    parity = dest & 1
    pos_ref[...] = dest * LANES + where % cap + cap * (parity ^ (group & 1))


def own_body(pick_ref, emb_ref, packed_ref):
    packed_ref[...] = jnp.dot(
        pick_ref[...], unit_of(emb_ref), preferred_element_type=F32
    ).astype(BF16)


def pack_body(cap, chips, emb_ref, code_ref, own, own_digits, *refs):
    group = lax.axis_index("group")
    pieces = emb_ref.shape[1] // LANES
    pick, mate_digits, _, _ = picked(code_ref, group >> 1, group & 1, chips, cap)
    mate = jnp.dot(pick, unit_of(emb_ref), preferred_element_type=F32).astype(BF16)
    for s in range(chips):
        part = slice(s * cap, (s + 1) * cap)
        for k in range(pieces):
            lanes = slice(k * LANES, (k + 1) * LANES)
            refs[s][k * LANES : k * LANES + cap, :] = own[part, lanes]
            refs[s][k * LANES + cap : (k + 1) * LANES, :] = mate[part, lanes]
        refs[s][pieces * LANES : pieces * LANES + META, :] = jnp.concatenate(
            [own_digits[:META, part], mate_digits[:META, part]], axis=1
        ).astype(BF16)


def join_body(*refs):
    out_ref, base = refs[-1], 0
    for ref in refs[:-1]:
        out_ref[base : base + ref.shape[0], :] = ref[...]
        base += ref.shape[0]


def unfold(refs, pieces, x_ref, turned_ref, column_ref, row_ref):
    size = pieces * LANES + META
    base = 0
    for ref in refs:
        for b in range(ref.shape[0] // size):
            rows = slice(base, base + LANES)
            for k in range(pieces):
                lanes = slice(k * LANES, (k + 1) * LANES)
                piece = ref[b * size + k * LANES : b * size + (k + 1) * LANES, :]
                x_ref[rows, lanes] = piece
                if turned_ref is not None:
                    turned_ref[lanes, rows] = jnp.transpose(piece)
            meta = ref[b * size + pieces * LANES : (b + 1) * size, :].astype(F32)
            rank = meta[0:1, :] * 256.0 + meta[1:2, :]
            row_ref[:, rows] = rank
            column_ref[rows, :] = jnp.transpose(jnp.broadcast_to(rank, (LANES, LANES)))
            base += LANES


def wide_max(scores):
    return jnp.max(scores.reshape(-1, 8, scores.shape[1]), axis=0)


def lane_max(scores):
    parts = [scores[:, i : i + LANES] for i in range(0, scores.shape[1], LANES)]
    return functools.reduce(jnp.maximum, parts)


def across(column, width):
    return jnp.concatenate([column] * (width // LANES), axis=1)


def fold(keys_ref, rank_ref, best_ref, side_ref, query_ref, query_rank, turned):
    queries = query_rank.shape[1]
    tall = next(t for t in (512, 256, 128) if keys_ref.shape[0] % t == 0)
    wide = next(t for t in (256, 128) if queries % t == 0)

    def outer(i, _):
        mine = span(i, wide)

        def inner(j, _):
            keys = span(j, tall)
            if turned:
                scores = jnp.dot(
                    keys_ref[keys, :], query_ref[:, mine], preferred_element_type=F32
                )
            else:
                scores = nt(keys_ref[keys, :], query_ref[mine, :])
            earlier = across(rank_ref[keys, :], wide) < query_rank[:, mine]
            best_ref[:, mine] = jnp.maximum(
                best_ref[:, mine], wide_max(jnp.where(earlier, scores, -1.0))
            )
            if turned:
                side_ref[keys, :] = jnp.maximum(
                    side_ref[keys, :], lane_max(jnp.where(earlier, -1.0, scores))
                )
            return 0

        loop(keys_ref.shape[0] // tall, inner)
        return 0

    loop(queries // wide, outer)


def span(i, size):
    if isinstance(i, int):
        return slice(i * size, (i + 1) * size)
    return pl.ds(pl.multiple_of(i * size, size), size)


def loop(count, body):
    if count <= 4:
        for i in range(count):
            body(i, 0)
    else:
        lax.fori_loop(0, count, body, 0)


def stage_body(pieces, olds, many, places, sources, *refs):
    refs = list(refs)

    def take(n):
        taken = refs[:n]
        del refs[:n]
        return taken

    xs, rows, blocks = take(olds), take(olds), take(many)
    found = take(sum(range(olds + 1))) if places else []
    if places:
        (out,) = take(1)
        news, turned_ref, (row_ref, best_ref) = take(olds), None, take(2)
    else:
        turned_ref, row_ref, best_ref = take(3)
        news = take(olds)
    x_ref, column_ref, side_ref = take(3)
    unfold(blocks, pieces, x_ref, turned_ref, column_ref, row_ref)
    best_ref[...] = jnp.full(best_ref.shape, -1.0, F32)
    side_ref[...] = jnp.full(side_ref.shape, -1.0, F32)
    for x, row, new in zip(xs, rows, news):
        new[...] = jnp.full(new.shape, -1.0, F32)
        fold(x_ref, column_ref, new, side_ref, x, row, True)
    fold(x_ref, column_ref, best_ref, side_ref, x_ref, row_ref, False)
    if not places:
        for i in range(0, x_ref.shape[0], LANES):
            side = jnp.transpose(side_ref[i : i + LANES, :])
            best_ref[:, i : i + LANES] = jnp.maximum(best_ref[:, i : i + LANES], wide_max(side))
        return
    planes = len(places)
    group = lax.axis_index("group")
    for p, place in enumerate(places):
        plane = jnp.where((group & 1) == 0, sources[0][p], sources[1][p])
        for s, (stage, block) in enumerate(place):
            lanes = slice(block * LANES, (block + 1) * LANES)
            if stage == olds:
                side = jnp.transpose(side_ref[lanes, :])
                best = jnp.maximum(best_ref[:, lanes], wide_max(side))
            else:
                best = news[stage][:, lanes]
                for later in range(stage, olds):
                    best = jnp.maximum(best, found[sum(range(later + 1)) + stage][:, lanes])
            best = jnp.max(best, axis=0, keepdims=True)
            device = ((group >> 1) ^ s) * 2 * planes + plane
            out[pl.ds(device, 1), :] = best
            out[pl.ds(device + planes, 1), :] = best


def final_body(planes, pos_ref, table_ref, out_ref):
    groups = table_ref.shape[0] // planes
    pos = pos_ref[...]
    rows = [g * planes + planes // 2 - 1 + (g & 1) for g in range(groups)]
    table = jnp.concatenate([table_ref[r : r + 1, :] for r in rows], axis=0)
    for i in range(0, pos.shape[1], LANES):
        here = jnp.broadcast_to(pos[:, i : i + LANES], (groups, LANES))
        got = jnp.take_along_axis(table, here % LANES, axis=1)
        mine = lax.broadcasted_iota(jnp.int32, here.shape, 0) == here // LANES
        out_ref[:, i : i + LANES] = jnp.sum(jnp.where(mine, got, 0.0), axis=0, keepdims=True)


def chunks_of(chips):
    away = list(range(1, chips))
    cuts = [len(away) * i // 3 for i in range(4)]
    return [[0]] + [away[a:b] for a, b in zip(cuts, cuts[1:])]


def on_device(embeddings, dest_group, order_rank):
    rows, width = embeddings.shape
    groups = lax.axis_size("group")
    planes = lax.axis_size("blk")
    chips, half = groups // 2, planes // 2
    cap = rows // 4
    pieces = width // LANES
    size = pieces * LANES + META

    def blocks(n):
        return jax.ShapeDtypeStruct((n * size, LANES), BF16)

    def floats(*shape):
        return jax.ShapeDtypeStruct(shape, F32)

    def to_chip(value, s):
        return lax.ppermute(value, "group", [(i, i ^ (2 * s)) for i in range(groups)])

    def to_core(value):
        return lax.ppermute(value, "group", [(i, i ^ 1) for i in range(groups)])

    meet = [half - 1, half]
    sources = [[z for z in range(planes) if z != half]]
    sources.insert(0, [planes - 1 - z for z in sources[0]])

    def meeting(step):
        return [
            (g * planes + sources[g & 1][step], g * planes + meet[g & 1]) for g in range(groups)
        ]

    def gather(value):
        arrived = [value]
        for step in range(planes - 1):
            arrived.append(lax.ppermute(value, ("group", "blk"), meeting(step)))
        return arrived

    code = jnp.concatenate([dest_group.reshape(1, rows), order_rank.reshape(1, rows)], axis=0)
    mate = to_core(embeddings)
    mate_code = to_core(code)
    flops = 2 * chips * cap * rows * width
    pick, own_digits, pos = call(
        functools.partial(index_body, cap, chips),
        [
            jax.ShapeDtypeStruct((chips * cap, rows), BF16),
            floats(2 * META, chips * cap),
            jax.ShapeDtypeStruct((1, rows), jnp.int32),
        ],
        [code],
        8 * flops,
        4 * rows * width,
        8 << 20,
    )
    own = call(
        own_body,
        jax.ShapeDtypeStruct((chips * cap, width), BF16),
        [pick, embeddings],
        flops,
        4 * rows * width,
        16 << 20,
    )
    packed = call(
        functools.partial(pack_body, cap, chips),
        [blocks(1)] * chips,
        [mate, mate_code, own, own_digits],
        flops,
        8 * rows * width,
        16 << 20,
    )
    sent = [packed[0]]
    for s in range(1, chips):
        sent.append(to_chip(packed[s], s))

    def join(arrays):
        if len(arrays) == 1:
            return arrays[0]
        total = sum(a.shape[0] for a in arrays)
        moved = 4 * total * LANES
        out = jax.ShapeDtypeStruct((total, LANES), BF16)
        return call(join_body, out, arrays, 1000, moved, 2 * moved)

    chunks = chunks_of(chips)
    arrived = []
    for chunk in chunks:
        arrived.append(gather(join([sent[s] for s in chunk])))
    stages = [[(c, p) for p in range(planes)] for c in range(len(chunks) - 1)]
    last = [(len(chunks) - 1, p) for p in range(planes)]
    stages += [last[:1] + last[1 + half :], last[1 : 1 + half]]
    places = [[None] * chips for _ in range(planes)]
    for i, stage in enumerate(stages):
        block = 0
        for c, p in stage:
            for s in chunks[c]:
                places[p][s] = (i, block)
                block += 1
    xs, ranks, found = [], [], []
    for i, stage in enumerate(stages):
        n = sum(len(chunks[c]) for c, _ in stage) * LANES
        count = n + sum(x.shape[1] for x in xs)
        flops = 2 * n * width * count
        made = [((width, n), BF16), ((1, n), F32), ((8, n), F32)]
        kept = [((8, x.shape[1]), F32) for x in xs]
        spare = [pltpu.VMEM((n, width), BF16)] + [pltpu.VMEM((n, LANES), F32)] * 2
        operands = xs + ranks + [arrived[c][p] for c, p in stage]
        if i == len(stages) - 1:
            operands += found
            outs = floats(groups * planes, LANES)
            spare = [pltpu.VMEM(*m) for m in kept + made[1:]] + spare
        else:
            outs = [jax.ShapeDtypeStruct(*m) for m in made + kept]
        best = call(
            functools.partial(
                stage_body,
                pieces,
                i,
                len(stage),
                places if i == len(stages) - 1 else None,
                [[meet[parity]] + sources[parity] for parity in range(2)],
            ),
            outs,
            operands,
            flops,
            2 * width * count,
            8 * width * 2 * n + (12 << 20),
            scratch=spare,
        )
        if i < len(stages) - 1:
            xs.append(best[0])
            ranks.append(best[1])
            found += best[3:] + best[2:3]
    table = lax.all_to_all(best, ("group", "blk"), 0, 0, tiled=True)
    final = functools.partial(final_body, planes)
    result = call(final, floats(1, rows), [pos, table], 1000000, 100000, 4 << 20)
    return result.reshape(rows)


def solution(mesh):
    placed = (P(("group", "blk"), None), P(("group", "blk"), None), P(("group", "blk")))

    return jax.shard_map(
        on_device, mesh=mesh, in_specs=placed, out_specs=P(("group", "blk")), check_vma=False
    )
```
